32 devices in a mesh: blk: 16 (over z, x, core), grp: 2 (over y).
Axes of the slice: x: 2, y: 2, z: 4, core: 2. Of those that a mesh axis runs over, the one named last changes fastest.
Arguments:
- embeddings: bfloat16 [32768, 1024], P(('blk', 'grp')), may hold values from -6 to 6
Outputs:
- tile_max: float32 [32768, 40], P(('blk', 'grp'))
The draws below stay inside these ranges and needn't reach their ends.
All inputs are finite; a program needn't handle non-finite values.
Results may differ from the reference program's by a relative error of at most 0.0017.
Values may be sent and summed in bfloat16 or wider, within the bound.
A program may use at most 64 MiB of HBM per device.

```python
import jax
import jax.numpy as jnp
from jax import lax

D = 1024
R_DEV = 1024
TILES = 8
BLOCKS = 32
ROWS = 32768


def steps_of(key, extent, split, least, largest):
    loudness = 1.0
    for axis_at, shards_of in split:
        heights = jax.random.uniform(jax.random.fold_in(jax.random.fold_in(key, 6), axis_at), (shards_of,), jnp.float32, least / len(split), largest / len(split))
        loudness = loudness * jnp.repeat(jnp.exp(heights), extent[axis_at] // shards_of).reshape((-1,) + (1,) * (len(extent) - 1 - axis_at))
    return loudness


def normal_values(own_key, dims, deviation, most, split=(), held_as=jnp.bfloat16):
    array = jax.random.normal(own_key, dims, jnp.float32) * deviation
    if len(split) > 0:
        array = steps_of(own_key, dims, split, -0.22, 0.18) * array
    return jnp.clip(array, min=-most, max=most).astype(held_as)


def setup_inputs(seed: int = 0) -> dict:
    splits = jax.random.split(jax.random.key(seed), 2)
    return {
        "embeddings": normal_values(splits[0], (ROWS, D), 1.0, 6.0, ((0, 32),)),
    }


def tile_rows(scores):
    count = scores.shape[0]
    return lax.optimization_barrier(jnp.max(scores.reshape(count, count // 128, 128), axis=-1))

def tile_columns(scores):
    count = scores.shape[0]
    return jnp.transpose(lax.optimization_barrier(jnp.max(scores.reshape(count // 128, 128, count), axis=1)))

def reference(embeddings):
    values = embeddings.astype(jnp.float32)
    unit = (values * lax.rsqrt(lax.optimization_barrier(jnp.mean(values * values, axis=-1, keepdims=True)) + 1e-06)).astype(jnp.bfloat16)
    blocks = unit.reshape(BLOCKS, R_DEV, D)
    next_one = jnp.roll(blocks, -1, axis=0)
    next_two = jnp.roll(blocks, -2, axis=0)
    scale = 1.0 / D ** 0.5
    same = jnp.arange(R_DEV)[:, None] == jnp.arange(R_DEV)[None, :]

    def score(queries, keys):
        return lax.dot_general(queries, keys, (((1,), (1,)), ((), ())), preferred_element_type=jnp.float32) * scale

    def per_block(triple):
        queries, first, second = triple
        own = jnp.where(same, -jnp.inf, score(queries, queries))
        one = score(queries, first)
        two = score(queries, second)
        return (tile_rows(own), tile_rows(one), tile_rows(two), tile_columns(one), tile_columns(two))
    own_max, one_max, two_max, col_one, col_two = lax.map(per_block, (blocks, next_one, next_two))
    back_one = jnp.roll(col_one, 1, axis=0)
    back_two = jnp.roll(col_two, 2, axis=0)
    joined = jnp.concatenate([back_two, back_one, own_max, one_max, two_max], axis=2)
    return joined.reshape(ROWS, 5 * TILES)
```

```python
import functools

import jax
import jax.numpy as jnp
from jax import lax
from jax.experimental import pallas as pl
from jax.experimental.pallas import tpu as pltpu
from jax.sharding import PartitionSpec as P

MESH = pl.DeviceIdType.MESH
CHUNKS = 4
TILE = 128


def unit_rows(raw):
    values = raw.astype(jnp.float32)
    mean = jnp.mean(values * values, axis=-1, keepdims=True)
    return (values * lax.rsqrt(mean + 1e-06)).astype(jnp.bfloat16)


def dot_nt(a, b):
    return lax.dot_general(a, b, (((1,), (1,)), ((), ())), preferred_element_type=jnp.float32)


def kernel(
    names, x_hbm, out_ref, x, u, got, relay, unit_c, res, tiles,
    in_sem, own_send, core_send, far_send, pass_send, relay_send, got_recv, relay_recv, res_send, res_recv,
):
    count, width = x.shape
    rows = count // CHUNKS
    per = rows // TILE
    half = CHUNKS // 2
    scale = 1.0 / width**0.5
    groups = lax.axis_size(names[1])
    total = lax.axis_size(names[0]) * groups
    me = lax.axis_index(names[0]) * groups + lax.axis_index(names[1])
    role = lax.rem(me, 4)
    odd = lax.rem(me // 4, 2)
    is_odd = odd == 1
    even = odd == 0

    def at(offset):
        block = lax.rem(me + offset + total, total)
        return (block // groups, lax.rem(block, groups))

    def pick(a, b, c, d):
        return jnp.where(role == 0, a, jnp.where(role == 1, b, jnp.where(role == 2, c, d)))

    def span(c):
        start = c * rows
        return pl.ds(start if isinstance(c, int) else pl.multiple_of(start, rows), rows)

    def link(src, dst, offset, send, recv):
        return pltpu.make_async_remote_copy(
            src_ref=src, dst_ref=dst, send_sem=send, recv_sem=recv,
            device_id=at(offset), device_id_type=MESH,
        )

    fetch = [
        pltpu.make_async_copy(x_hbm.at[span(c)], x.at[span(c)], in_sem.at[c]) for c in range(CHUNKS)
    ]
    for copy in fetch:
        copy.start()

    barrier = pltpu.get_barrier_semaphore()
    for offset in (-2, -1, 1, 2):
        pl.semaphore_signal(barrier, inc=1, device_id=at(offset), device_id_type=MESH)
    pl.semaphore_wait(barrier, 4)

    def own_copy(c):
        slot = jnp.where(role == 0, 1, 0)
        return link(
            x.at[span(c)], got.at[slot, span(c)], pick(-2, -1, 1, 2),
            own_send.at[c], got_recv.at[slot, c],
        )

    to_core = role >= 2

    def core_copy(c):
        return link(x.at[span(c)], got.at[1, span(c)], -2, core_send.at[c], got_recv.at[1, c])

    to_far = is_odd & ((role == 0) | (role == 3))

    def far_copy(j):
        return link(
            x.at[span(half + j)], relay.at[span(j)], jnp.where(role == 0, 1, -1),
            far_send.at[j], relay_recv.at[j],
        )

    through = is_odd & ((role == 1) | (role == 2))

    def relay_copy(j):
        return link(
            relay.at[span(j)], got.at[2, span(half + j)], jnp.where(role == 1, -2, 2),
            relay_send.at[j], got_recv.at[2, half + j],
        )

    def passes(s, c):
        return jnp.where(
            s == 0,
            (role == 0) | ((role == 1) & even & (c < half)),
            (s == 1) & (role == 2) & even & (c < half),
        )

    def pass_copy(s, c):
        slot = jnp.where(role == 0, 0, 2)
        return link(
            got.at[s, span(c)], got.at[slot, span(c)], pick(2, -1, 1, 1),
            pass_send.at[s, c], got_recv.at[slot, c],
        )

    def offset_of(s):
        return jnp.where(s == 0, pick(1, -2, -1, -1), jnp.where(s == 1, 2, jnp.where(role == 0, -1, 1)))

    def active(s):
        return (s == 0) | ((s == 1) & (role != 3)) | ((s == 2) & even & ((role == 0) | (role == 3)))

    def res_copy(s):
        offset = offset_of(s)
        return link(
            res.at[s], tiles.at[2 - offset], offset, res_send.at[s], res_recv.at[2 - offset],
        )

    for c in range(CHUNKS):
        fetch[c].wait()
        own_copy(c).start()

        @pl.when(to_core)
        def _():
            core_copy(c).start()

        if c >= half:

            @pl.when(to_far)
            def _():
                far_copy(c - half).start()

    def make_unit(c, carry):
        u[span(c), :] = unit_rows(x[span(c), :])
        return carry

    lax.fori_loop(0, CHUNKS, make_unit, 0)

    sub = lax.broadcasted_iota(jnp.int32, (per * CHUNKS, rows), 0)

    def put(place, c, j, scores):
        cols = pl.ds(j * rows, rows)
        held = tiles[place, :, cols]
        for t in range(per):
            top = jnp.max(scores[t * TILE : (t + 1) * TILE], axis=0, keepdims=True) * scale
            held = jnp.where(sub == c * per + t, top, held)
        tiles[place, :, cols] = held

    def own_scores(c, carry):
        mine = u[span(c), :]
        for j in range(CHUNKS):
            scores = dot_nt(mine, u[span(j), :])
            shift = (c - j) * rows
            same = (
                lax.broadcasted_iota(jnp.int32, scores.shape, 0) + shift
                == lax.broadcasted_iota(jnp.int32, scores.shape, 1)
            )
            put(2, c, j, jnp.where(same, -jnp.inf, scores))
        return carry

    lax.fori_loop(0, CHUNKS, own_scores, 0)

    def step(t, carry):
        late = t >= 2 * CHUNKS
        place = t - 2 * CHUNKS
        s = jnp.where(late, 2, lax.rem(t, 2))
        c = jnp.where(late, jnp.where(lax.rem(place, 2) == 0, half, 0) + place // 2, t // 2)

        for j in range(half):

            @pl.when(through & (t == 2 + 2 * j))
            def _():
                link(
                    relay.at[span(j)], relay.at[span(j)], 1, far_send.at[j], relay_recv.at[j]
                ).wait_recv()
                relay_copy(j).start()

        @pl.when(active(s))
        def _():
            link(
                got.at[s, span(c)], got.at[s, span(c)], 1, own_send.at[0], got_recv.at[s, c]
            ).wait_recv()

            @pl.when(passes(s, c))
            def _():
                pass_copy(s, c).start()

            unit_c[...] = unit_rows(got[s, span(c), :])
            theirs = unit_c[...]
            cols = span(c)
            for j in range(CHUNKS):
                scores = dot_nt(u[span(j), :], theirs)
                for i in range(per):
                    top = jnp.max(scores[i * TILE : (i + 1) * TILE], axis=0, keepdims=True) * scale
                    res[s, pl.ds(j * per + i, 1), cols] = top
            offset = offset_of(s)
            for j in range(CHUNKS):
                put(offset + 2, c, j, dot_nt(theirs, u[span(j), :]))

            last = (t == 2 * CHUNKS - 2) | (t == 2 * CHUNKS - 1) | (t == 3 * CHUNKS - 1)

            @pl.when(last)
            def _():
                res_copy(s).start()

        return carry

    lax.fori_loop(0, 3 * CHUNKS, step, 0)

    for c in range(CHUNKS):
        own_copy(c).wait_send()

        @pl.when(to_core)
        def _():
            core_copy(c).wait_send()

        for s in range(2):

            @pl.when(passes(s, c))
            def _():
                pass_copy(s, c).wait_send()

    for j in range(half):

        @pl.when(to_far)
        def _():
            far_copy(j).wait_send()

        @pl.when(through)
        def _():
            relay_copy(j).wait_send()

    for s in range(3):

        @pl.when(active(s))
        def _():
            res_copy(s).wait_send()

    for offset in (-2, -1, 1, 2):
        here = jnp.bool_(False)
        for s in range(3):
            here = here | (active(s) & (offset_of(s) == offset))

        @pl.when(jnp.logical_not(here))
        def _():
            link(
                res.at[0], tiles.at[offset + 2], offset, res_send.at[0], res_recv.at[offset + 2]
            ).wait_recv()

    for i in range(5):
        out_ref[pl.ds(i * per * CHUNKS, per * CHUNKS), :] = tiles[i]


def body(names, embeddings):
    count, width = embeddings.shape
    tiles = count // TILE
    rows = count // CHUNKS
    half = CHUNKS // 2
    bf16 = embeddings.dtype
    dma = pltpu.SemaphoreType.DMA
    wide = pl.pallas_call(
        functools.partial(kernel, names),
        out_shape=jax.ShapeDtypeStruct((5 * tiles, count), jnp.float32),
        in_specs=[pl.BlockSpec(memory_space=pl.ANY)],
        out_specs=pl.BlockSpec(memory_space=pltpu.VMEM),
        scratch_shapes=[
            pltpu.VMEM((count, width), bf16),
            pltpu.VMEM((count, width), bf16),
            pltpu.VMEM((3, count, width), bf16),
            pltpu.VMEM((count // 2, width), bf16),
            pltpu.VMEM((rows, width), bf16),
            pltpu.VMEM((3, tiles, count), jnp.float32),
            pltpu.VMEM((5, tiles, count), jnp.float32),
            dma((CHUNKS,)),
            dma((CHUNKS,)),
            dma((CHUNKS,)),
            dma((half,)),
            dma((2, CHUNKS)),
            dma((half,)),
            dma((3, CHUNKS)),
            dma((half,)),
            dma((3,)),
            dma((5,)),
        ],
        compiler_params=pltpu.CompilerParams(
            collective_id=0, has_side_effects=True, vmem_limit_bytes=60 * 1024 * 1024
        ),
    )(embeddings)
    return jnp.transpose(wide)


def solution(mesh):
    names = ("blk", "grp")
    return jax.shard_map(
        functools.partial(body, names),
        mesh=mesh,
        in_specs=(P(names, None),),
        out_specs=P(names, None),
        check_vma=False,
    )
```

```python
import functools

import jax
import jax.numpy as jnp
from jax import lax
from jax.experimental import pallas as pl
from jax.experimental.pallas import tpu as pltpu
from jax.sharding import PartitionSpec as P

MESH = pl.DeviceIdType.MESH
CHUNKS = 4
TILE = 128


def unit_rows(raw):
    values = raw.astype(jnp.float32)
    mean = jnp.mean(values * values, axis=-1, keepdims=True)
    return (values * lax.rsqrt(mean + 1e-06)).astype(jnp.bfloat16)


def dot_nt(a, b):
    return lax.dot_general(a, b, (((1,), (1,)), ((), ())), preferred_element_type=jnp.float32)


def kernel(
    names, x_hbm, out_ref, x, u, got, relay, unit_c, res, tiles,
    in_sem, own_send, core_send, far_send, pass_send, relay_send, got_recv, relay_recv, res_send, res_recv,
):
    count, width = x.shape
    rows = count // CHUNKS
    per = rows // TILE
    half = CHUNKS // 2
    scale = 1.0 / width**0.5
    groups = lax.axis_size(names[1])
    total = lax.axis_size(names[0]) * groups
    me = lax.axis_index(names[0]) * groups + lax.axis_index(names[1])
    role = lax.rem(me, 4)
    odd = lax.rem(me // 4, 2)
    is_odd = odd == 1
    even = odd == 0

    def at(offset):
        block = lax.rem(me + offset + total, total)
        return (block // groups, lax.rem(block, groups))

    def pick(a, b, c, d):
        return jnp.where(role == 0, a, jnp.where(role == 1, b, jnp.where(role == 2, c, d)))

    def span(c):
        start = c * rows
        return pl.ds(start if isinstance(c, int) else pl.multiple_of(start, rows), rows)

    def link(src, dst, offset, send, recv):
        return pltpu.make_async_remote_copy(
            src_ref=src, dst_ref=dst, send_sem=send, recv_sem=recv,
            device_id=at(offset), device_id_type=MESH,
        )

    fetch = [
        pltpu.make_async_copy(x_hbm.at[span(c)], x.at[span(c)], in_sem.at[c]) for c in range(CHUNKS)
    ]
    for copy in fetch:
        copy.start()

    barrier = pltpu.get_barrier_semaphore()
    for offset in (-2, -1, 1, 2):
        pl.semaphore_signal(barrier, inc=1, device_id=at(offset), device_id_type=MESH)
    pl.semaphore_wait(barrier, 4)

    def own_copy(c):
        slot = jnp.where(role == 0, 1, 0)
        return link(
            x.at[span(c)], got.at[slot, span(c)], pick(-2, -1, 1, 2),
            own_send.at[c], got_recv.at[slot, c],
        )

    to_core = role >= 2

    def core_copy(c):
        return link(x.at[span(c)], got.at[1, span(c)], -2, core_send.at[c], got_recv.at[1, c])

    to_far = is_odd & ((role == 0) | (role == 3))

    def far_copy(j):
        return link(
            x.at[span(half + j)], relay.at[span(j)], jnp.where(role == 0, 1, -1),
            far_send.at[j], relay_recv.at[j],
        )

    through = is_odd & ((role == 1) | (role == 2))

    def relay_copy(j):
        return link(
            relay.at[span(j)], got.at[2, span(half + j)], jnp.where(role == 1, -2, 2),
            relay_send.at[j], got_recv.at[2, half + j],
        )

    def passes(s, c):
        return jnp.where(
            s == 0,
            (role == 0) | ((role == 1) & even & (c < half)),
            (s == 1) & (role == 2) & even & (c < half),
        )

    def pass_copy(s, c):
        slot = jnp.where(role == 0, 0, 2)
        return link(
            got.at[s, span(c)], got.at[slot, span(c)], pick(2, -1, 1, 1),
            pass_send.at[s, c], got_recv.at[slot, c],
        )

    def offset_of(s):
        return jnp.where(s == 0, pick(1, -2, -1, -1), jnp.where(s == 1, 2, jnp.where(role == 0, -1, 1)))

    def active(s):
        return (s == 0) | ((s == 1) & (role != 3)) | ((s == 2) & even & ((role == 0) | (role == 3)))

    def res_copy(s):
        offset = offset_of(s)
        return link(
            res.at[s], tiles.at[2 - offset], offset, res_send.at[s], res_recv.at[2 - offset],
        )

    for c in range(CHUNKS):
        fetch[c].wait()
        own_copy(c).start()

        @pl.when(to_core)
        def _():
            core_copy(c).start()

        if c >= half:

            @pl.when(to_far)
            def _():
                far_copy(c - half).start()

    def make_unit(c, carry):
        u[span(c), :] = unit_rows(x[span(c), :])
        return carry

    lax.fori_loop(0, CHUNKS, make_unit, 0)

    sub = lax.broadcasted_iota(jnp.int32, (per * CHUNKS, rows), 0)

    def put(place, c, j, scores):
        cols = pl.ds(j * rows, rows)
        held = tiles[place, :, cols]
        for t in range(per):
            top = jnp.max(scores[t * TILE : (t + 1) * TILE], axis=0, keepdims=True) * scale
            held = jnp.where(sub == c * per + t, top, held)
        tiles[place, :, cols] = held

    def own_scores(c, carry):
        mine = u[span(c), :]
        for j in range(CHUNKS):
            scores = dot_nt(mine, u[span(j), :])
            shift = (c - j) * rows
            same = (
                lax.broadcasted_iota(jnp.int32, scores.shape, 0) + shift
                == lax.broadcasted_iota(jnp.int32, scores.shape, 1)
            )
            put(2, c, j, jnp.where(same, -jnp.inf, scores))
        return carry

    lax.fori_loop(0, CHUNKS, own_scores, 0)

    flip = jnp.where(role == 2, 1, 0)

    def step(t, carry):
        late = t >= 2 * CHUNKS
        place = t - 2 * CHUNKS
        s = jnp.where(late, 2, lax.rem(t + flip, 2))
        c = jnp.where(late, jnp.where(lax.rem(place, 2) == 0, half, 0) + place // 2, t // 2)

        for j in range(half):

            @pl.when(through & (t == 1 + 2 * j))
            def _():
                link(
                    relay.at[span(j)], relay.at[span(j)], 1, far_send.at[j], relay_recv.at[j]
                ).wait_recv()
                relay_copy(j).start()

        @pl.when(active(s))
        def _():
            link(
                got.at[s, span(c)], got.at[s, span(c)], 1, own_send.at[0], got_recv.at[s, c]
            ).wait_recv()

            @pl.when(passes(s, c))
            def _():
                pass_copy(s, c).start()

            unit_c[...] = unit_rows(got[s, span(c), :])
            theirs = unit_c[...]
            cols = span(c)
            for j in range(CHUNKS):
                scores = dot_nt(u[span(j), :], theirs)
                for i in range(per):
                    top = jnp.max(scores[i * TILE : (i + 1) * TILE], axis=0, keepdims=True) * scale
                    res[s, pl.ds(j * per + i, 1), cols] = top
            last = (t == 2 * CHUNKS - 2) | (t == 2 * CHUNKS - 1) | (t == 3 * CHUNKS - 1)

            @pl.when(last)
            def _():
                res_copy(s).start()

            offset = offset_of(s)
            for j in range(CHUNKS):
                put(offset + 2, c, j, dot_nt(theirs, u[span(j), :]))

        return carry

    lax.fori_loop(0, 3 * CHUNKS, step, 0)

    for c in range(CHUNKS):
        own_copy(c).wait_send()

        @pl.when(to_core)
        def _():
            core_copy(c).wait_send()

        for s in range(2):

            @pl.when(passes(s, c))
            def _():
                pass_copy(s, c).wait_send()

    for j in range(half):

        @pl.when(to_far)
        def _():
            far_copy(j).wait_send()

        @pl.when(through)
        def _():
            relay_copy(j).wait_send()

    for s in range(3):

        @pl.when(active(s))
        def _():
            res_copy(s).wait_send()

    for offset in (-2, -1, 1, 2):
        here = jnp.bool_(False)
        for s in range(3):
            here = here | (active(s) & (offset_of(s) == offset))

        @pl.when(jnp.logical_not(here))
        def _():
            link(
                res.at[0], tiles.at[offset + 2], offset, res_send.at[0], res_recv.at[offset + 2]
            ).wait_recv()

    for i in range(5):
        out_ref[pl.ds(i * per * CHUNKS, per * CHUNKS), :] = tiles[i]


def body(names, embeddings):
    count, width = embeddings.shape
    tiles = count // TILE
    rows = count // CHUNKS
    half = CHUNKS // 2
    bf16 = embeddings.dtype
    dma = pltpu.SemaphoreType.DMA
    wide = pl.pallas_call(
        functools.partial(kernel, names),
        out_shape=jax.ShapeDtypeStruct((5 * tiles, count), jnp.float32),
        in_specs=[pl.BlockSpec(memory_space=pl.ANY)],
        out_specs=pl.BlockSpec(memory_space=pltpu.VMEM),
        scratch_shapes=[
            pltpu.VMEM((count, width), bf16),
            pltpu.VMEM((count, width), bf16),
            pltpu.VMEM((3, count, width), bf16),
            pltpu.VMEM((count // 2, width), bf16),
            pltpu.VMEM((rows, width), bf16),
            pltpu.VMEM((3, tiles, count), jnp.float32),
            pltpu.VMEM((5, tiles, count), jnp.float32),
            dma((CHUNKS,)),
            dma((CHUNKS,)),
            dma((CHUNKS,)),
            dma((half,)),
            dma((2, CHUNKS)),
            dma((half,)),
            dma((3, CHUNKS)),
            dma((half,)),
            dma((3,)),
            dma((5,)),
        ],
        compiler_params=pltpu.CompilerParams(
            collective_id=0, has_side_effects=True, vmem_limit_bytes=60 * 1024 * 1024
        ),
    )(embeddings)
    return jnp.transpose(wide)


def solution(mesh):
    names = ("blk", "grp")
    return jax.shard_map(
        functools.partial(body, names),
        mesh=mesh,
        in_specs=(P(names, None),),
        out_specs=P(names, None),
        check_vma=False,
    )
```
